32 devices in a mesh: shard: 2 (over core), cols: 4 (over y, x), job: 4 (over z).
Axes of the slice: x: 2, y: 2, z: 4, core: 2. Of those that a mesh axis runs over, the one named last changes fastest.
Arguments:
- one_query: float32 [16384, 4096], P(('job', 'shard'), 'cols'), parts along dimension 0, may hold values from -0.125 to 0.125
- other_query: float32 [16384, 4096], P(('job', 'shard'), 'cols'), parts along dimension 0, may hold values from -0.09375 to 0.09375
- one_key: float32 [16384, 1024], P(('job', 'shard'), 'cols'), parts along dimension 0, may hold values from -0.125 to 0.125
- other_key: float32 [16384, 1024], P(('job', 'shard'), 'cols'), parts along dimension 0, may hold values from -0.09375 to 0.09375
- one_value: float32 [16384, 1024], P(('job', 'shard'), 'cols'), parts along dimension 0, may hold values from -0.125 to 0.125
- other_value: float32 [16384, 1024], P(('job', 'shard'), 'cols'), parts along dimension 0, may hold values from -0.09375 to 0.09375
- mix_share: float32 [16384], P(('job', 'shard')), parts along dimension 0, may hold values from 0.2 to 0.8
- norm_gain: float32 [16384], P(('job', 'shard')), parts along dimension 0, may hold values from 0.25 to 1.75
Outputs:
- final_query: bfloat16 [16384, 4096], P('job', 'cols'), parts along dimension 0
- final_key: bfloat16 [16384, 1024], P('job', 'cols'), parts along dimension 0
- final_value: bfloat16 [16384, 1024], P('job', 'cols'), parts along dimension 0
- scale_query: float32 [16384], P(('job', 'cols')), parts along dimension 0
- scale_key: float32 [4096], P(('job', 'cols')), parts along dimension 0
- scale_value: float32 [4096], P(('job', 'cols')), parts along dimension 0
The draws below stay inside these ranges and needn't reach their ends.
There are 4 independent parts, one for each index of `job`. The reference program is written for one: setup_inputs(seed, part) draws one part's arguments, and reference() takes and returns one part's arrays. A program takes and returns all parts, laid end to end along the dimension named above; each array names one. Nothing has to cross between parts.
All inputs are finite; a program needn't handle non-finite values. Where the reference program divides by a largest or mean magnitude, that divisor is 1e-20 or more.
Results may differ from the reference program's by a relative error of at most 0.001.
Values may be sent and summed in bfloat16 or wider, within the bound.
A program may use at most 128 MiB of HBM per device.

```python
import jax
import jax.numpy as jnp

D_MODEL = 4096
Q_DIM = 4096
KV_DIM = 1024


def strengthened(drawn, rng, source, target, blocks, factor):
    def block_of(position):
        return (jnp.arange(drawn.shape[position]) // (drawn.shape[position] // blocks)).reshape((-1,) + (1,) * (drawn.ndim - 1 - position))

    one_side = jax.random.permutation(rng, blocks)[block_of(target)]
    second = (block_of(target) + blocks // 2) % blocks
    return jnp.where((block_of(source) == one_side) | (block_of(source) == second), factor * drawn, drawn)


def level_of(own_key, shape, shards, smallest, high):
    def one(position, blocks):
        steps = jax.random.uniform(jax.random.fold_in(jax.random.fold_in(own_key, 6), position), (blocks,), jnp.float32, smallest / len(shards), high / len(shards))
        return jnp.repeat(jnp.exp(steps), shape[position] // blocks).reshape((-1,) + (1,) * (len(shape) - position - 1))

    factor_of = one(*shards[0])
    for cut in shards[1:]:
        factor_of = factor_of * one(*cut)
    return factor_of


def normal_values(key, shape, width, most, cuts=(), dtype=jnp.bfloat16):
    array = width * jax.random.normal(key, shape, jnp.float32)
    if cuts:
        array = array * level_of(key, shape, cuts, -0.22, 0.18)
    return jnp.clip(array, -most, most).astype(dtype)


def noise_with(stream_key, shape, scale, bound, pieces, heavy, dtype=jnp.bfloat16):
    entries = scale * jax.random.normal(stream_key, shape, jnp.float32)
    if pieces:
        entries = entries * level_of(stream_key, shape, pieces, -0.22, 0.18)
    return jnp.clip(strengthened(entries, jax.random.fold_in(stream_key, 3), *heavy), -bound, bound).astype(dtype)


def setup_inputs(seed: int = 0, part: int = 0) -> dict:
    arg_keys = jax.random.split(jax.random.key(seed), 9)
    part_keys = jax.random.split(jax.random.fold_in(arg_keys[8], part), 9)
    return {
        "one_query": noise_with(part_keys[0], (D_MODEL, Q_DIM), D_MODEL ** -0.5, 0.125, ((0, 2), (1, 4)), (0, 1, 4, 2.0), jnp.float32),
        "other_query": normal_values(part_keys[1], (D_MODEL, Q_DIM), D_MODEL ** -0.5, 0.09375, ((0, 2), (1, 4)), jnp.float32),
        "one_key": noise_with(part_keys[2], (D_MODEL, KV_DIM), D_MODEL ** -0.5, 0.125, ((0, 2), (1, 4)), (0, 1, 4, 2.0), jnp.float32),
        "other_key": normal_values(part_keys[3], (D_MODEL, KV_DIM), D_MODEL ** -0.5, 0.09375, ((0, 2), (1, 4)), jnp.float32),
        "one_value": noise_with(part_keys[4], (D_MODEL, KV_DIM), D_MODEL ** -0.5, 0.125, ((0, 2), (1, 4)), (0, 1, 4, 2.0), jnp.float32),
        "other_value": normal_values(part_keys[5], (D_MODEL, KV_DIM), D_MODEL ** -0.5, 0.09375, ((0, 2), (1, 4)), jnp.float32),
        "mix_share": jnp.clip(0.2 + 0.6 * jax.random.uniform(part_keys[6], (D_MODEL,), jnp.float32) ** level_of(part_keys[6], (D_MODEL,), ((0, 2),), -0.2, 0.2), 0.2, 0.8),
        "norm_gain": jnp.clip(1.0 + 0.15 * jax.random.normal(part_keys[7], (D_MODEL,), jnp.float32), 0.25, 1.75),
    }


def reference(one_query, other_query, one_key, other_key, one_value, other_value, mix_share, norm_gain):
    result_query = mix_share[:, None] * one_query + (1.0 - mix_share[:, None]) * other_query
    result_key = mix_share[:, None] * one_key + (1.0 - mix_share[:, None]) * other_key
    result_value = mix_share[:, None] * one_value + (1.0 - mix_share[:, None]) * other_value
    result_gained_query = result_query * norm_gain[:, None]
    result_gained_key = result_key * norm_gain[:, None]
    result_gained_value = result_value * norm_gain[:, None]
    scale_query = jnp.max(jnp.abs(result_gained_query), axis=0)
    final_query = (result_gained_query / scale_query).astype(jnp.bfloat16)
    scale_key = jnp.max(jnp.abs(result_gained_key), axis=0)
    final_key = (result_gained_key / scale_key).astype(jnp.bfloat16)
    scale_value = jnp.max(jnp.abs(result_gained_value), axis=0)
    final_value = (result_gained_value / scale_value).astype(jnp.bfloat16)
    return final_query, final_key, final_value, scale_query, scale_key, scale_value
```

```python
import functools

import jax
import jax.numpy as jnp
from jax import lax
from jax.experimental import pallas as pl
from jax.experimental.pallas import tpu as pltpu
from jax.sharding import PartitionSpec as P

LANES = 128
WIDTH = 128
BLOCK = 128
MESH = pl.DeviceIdType.MESH


def merge(n, chunks, *refs):
    ones, others = refs[0:3], refs[3:6]
    mix_hbm, gain_hbm = refs[6:8]
    finals, scales = refs[8:11], refs[11:14]
    held, extra = refs[14:17], refs[17:20]
    mix_ref, gain_ref, first, second, peaks = refs[20:25]
    row_sem, in_sem, peak_send, peak_recv, send_sem, recv_sem = refs[25:]
    me = lax.axis_index("shard")
    rows = held[0].shape[0]
    peers = [lax.rem(me + k, n) for k in range(1, n)]

    def loads(c):
        a, col = chunks[c]
        cols = pl.ds(col, WIDTH)
        return (
            pltpu.make_async_copy(ones[a].at[:, cols], held[a].at[:, cols], in_sem.at[c, 0]),
            pltpu.make_async_copy(others[a].at[:, cols], extra[a].at[:, cols], in_sem.at[c, 1]),
        )

    def peak_copy(c, k, slot):
        return pltpu.make_async_remote_copy(
            src_ref=peaks.at[c, slot],
            dst_ref=peaks.at[c, slot],
            send_sem=peak_send.at[c, k],
            recv_sem=peak_recv.at[c, slot],
            device_id={"shard": peers[k]},
            device_id_type=MESH,
        )

    def block_copy(c, k, slot):
        a, col = chunks[c]
        block = finals[a].at[pl.ds(pl.multiple_of(slot * rows, rows), rows), pl.ds(col, WIDTH)]
        return pltpu.make_async_remote_copy(
            src_ref=block,
            dst_ref=block,
            send_sem=send_sem.at[c, k],
            recv_sem=recv_sem.at[c, slot],
            device_id={"shard": peers[k]},
            device_id_type=MESH,
        )

    factors = (
        pltpu.make_async_copy(mix_hbm, mix_ref, row_sem.at[0]),
        pltpu.make_async_copy(gain_hbm, gain_ref, row_sem.at[1]),
    )
    for copy in factors:
        copy.start()
    for c in range(len(chunks)):
        for copy in loads(c):
            copy.start()

    barrier = pltpu.get_barrier_semaphore()
    for peer in peers:
        pl.semaphore_signal(barrier, inc=1, device_id={"shard": peer}, device_id_type=MESH)

    for copy in factors:
        copy.wait()
    for k in range(rows // LANES):
        mix = mix_ref[k : k + 1, :]
        gain = gain_ref[k : k + 1, :]
        span = pl.ds(k * LANES, LANES)
        first[span, :] = jnp.broadcast_to(mix * gain, (LANES, LANES)).T
        second[span, :] = jnp.broadcast_to((1.0 - mix) * gain, (LANES, LANES)).T

    pl.semaphore_wait(barrier, n - 1)

    def combine(c):
        a, col = chunks[c]
        for copy in loads(c):
            copy.wait()
        cols = pl.ds(col, WIDTH)

        def step(i, peak):
            span = pl.ds(pl.multiple_of(i * BLOCK, BLOCK), BLOCK)
            value = first[span, :] * held[a][span, cols] + second[span, :] * extra[a][span, cols]
            held[a][span, cols] = value
            return jnp.maximum(peak, jnp.max(jnp.abs(value).reshape(BLOCK // 8, 8, WIDTH), axis=0))

        peaks[c, me] = lax.fori_loop(0, rows // BLOCK, step, jnp.zeros((8, WIDTH), jnp.float32))
        for k in range(n - 1):
            peak_copy(c, k, me).start()

    def finish(c):
        a, col = chunks[c]
        cols = pl.ds(col, WIDTH)
        for k in range(n - 1):
            peak_copy(c, k, peers[k]).wait_recv()
        peak = peaks[c, 0]
        for k in range(1, n):
            peak = jnp.maximum(peak, peaks[c, k])
        scale = jnp.max(peak, axis=0, keepdims=True)
        row = col // LANES
        scales[a][row : row + 1, :] = scale
        inverse = 1.0 / scale

        def step(i, carry):
            span = pl.ds(pl.multiple_of(i * BLOCK, BLOCK), BLOCK)
            out = pl.ds(pl.multiple_of(me * rows + i * BLOCK, BLOCK), BLOCK)
            finals[a][out, cols] = (held[a][span, cols] * inverse).astype(jnp.bfloat16)
            return carry

        lax.fori_loop(0, rows // BLOCK, step, 0)
        for k in range(n - 1):
            block_copy(c, k, me).start()

    combine(0)
    for c in range(len(chunks)):
        if c + 1 < len(chunks):
            combine(c + 1)
        finish(c)
    for c in range(len(chunks)):
        for k in range(n - 1):
            peak_copy(c, k, me).wait_send()
            block_copy(c, k, me).wait_send()
            block_copy(c, k, peers[k]).wait_recv()


def write_out(*refs):
    half = (len(refs) - 1) // 2
    sem = refs[-1]
    copies = [
        pltpu.make_async_copy(refs[i], refs[half + i], sem.at[i]) for i in range(half)
    ]
    for copy in copies:
        copy.start()
    for copy in copies:
        copy.wait()


def shards(
    n, one_query, other_query, one_key, other_key, one_value, other_value, mix_share, norm_gain
):
    ones = (one_query, one_key, one_value)
    others = (other_query, other_key, other_value)
    rows = one_query.shape[0]
    chunks = [(a, col) for a in range(3) for col in range(0, ones[a].shape[1], WIDTH)]
    count = len(chunks)
    vmem = pl.BlockSpec(memory_space=pltpu.VMEM)
    hbm = pl.BlockSpec(memory_space=pltpu.HBM)
    shapes = [((n * rows, x.shape[1]), jnp.bfloat16) for x in ones] + [
        ((x.shape[1] // LANES, LANES), jnp.float32) for x in ones
    ]
    scratch = (
        [pltpu.VMEM(x.shape, jnp.float32) for x in ones + others]
        + [pltpu.VMEM((rows // LANES, LANES), jnp.float32)] * 2
        + [pltpu.VMEM((rows, LANES), jnp.float32)] * 2
        + [
            pltpu.VMEM((count, n, 8, WIDTH), jnp.float32),
            pltpu.SemaphoreType.DMA((2,)),
            pltpu.SemaphoreType.DMA((count, 2)),
            pltpu.SemaphoreType.DMA((count, n - 1)),
            pltpu.SemaphoreType.DMA((count, n)),
            pltpu.SemaphoreType.DMA((count, n - 1)),
            pltpu.SemaphoreType.DMA((count, n)),
        ]
    )
    grant = sum(2 * x.size * 4 for x in ones) + 2 * rows * LANES * 4
    grant += count * n * 8 * WIDTH * 4 + (2 << 20)
    merged = pl.pallas_call(
        functools.partial(merge, n, chunks),
        out_shape=[pltpu.VMEM(s, d) for s, d in shapes],
        in_specs=[hbm] * 8,
        out_specs=[vmem] * 6,
        scratch_shapes=scratch,
        compiler_params=pltpu.CompilerParams(
            collective_id=0, has_side_effects=True, vmem_limit_bytes=grant
        ),
        name="merge",
    )(
        *(
            pltpu.with_memory_space_constraint(x, pltpu.HBM)
            for x in (
                *ones,
                *others,
                mix_share.reshape(rows // LANES, LANES),
                norm_gain.reshape(rows // LANES, LANES),
            )
        )
    )
    outs = pl.pallas_call(
        write_out,
        out_shape=[jax.ShapeDtypeStruct(s, d) for s, d in shapes],
        in_specs=[vmem] * 6,
        out_specs=[hbm] * 6,
        scratch_shapes=[pltpu.SemaphoreType.DMA((6,))],
        compiler_params=pltpu.CompilerParams(vmem_limit_bytes=1 << 20),
        name="write_out",
    )(*merged)
    return (*outs[:3], *(x.reshape(-1) for x in outs[3:]))


def solution(mesh):
    rows = P(("job", "shard"))
    blocks = P(("job", "shard"), "cols")
    return jax.shard_map(
        functools.partial(shards, mesh.shape["shard"]),
        mesh=mesh,
        in_specs=(blocks,) * 6 + (rows,) * 2,
        out_specs=(P("job", "cols"),) * 3 + (P(("job", "cols")),) * 3,
        check_vma=False,
    )
```

```python
import functools

import jax
import jax.numpy as jnp
from jax import lax
from jax.experimental import pallas as pl
from jax.experimental.pallas import tpu as pltpu
from jax.sharding import PartitionSpec as P

LANES = 128
NARROW = 2
WIDTH = 256
BLOCK = 512
MESH = pl.DeviceIdType.MESH


def merge(n, chunks, *refs):
    ones, others = refs[0:3], refs[3:6]
    mix_hbm, gain_hbm = refs[6:8]
    finals, scales = refs[8:11], refs[11:14]
    held, extra = refs[14:17], refs[17:20]
    mix_ref, gain_ref, first, second, peaks = refs[20:25]
    row_sem, in_sem, peak_send, peak_recv, send_sem, recv_sem = refs[25:]
    me = lax.axis_index("shard")
    rows = held[0].shape[0]
    peers = [lax.rem(me + k, n) for k in range(1, n)]

    def loads(c):
        a, col, width = chunks[c]
        cols = pl.ds(col, width)
        return (
            pltpu.make_async_copy(ones[a].at[:, cols], held[a].at[:, cols], in_sem.at[c, 0]),
            pltpu.make_async_copy(others[a].at[:, cols], extra[a].at[:, cols], in_sem.at[c, 1]),
        )

    def peak_copy(c, k, slot):
        width = chunks[c][2]
        return pltpu.make_async_remote_copy(
            src_ref=peaks.at[c, slot, :, pl.ds(0, width)],
            dst_ref=peaks.at[c, slot, :, pl.ds(0, width)],
            send_sem=peak_send.at[c, k],
            recv_sem=peak_recv.at[c, slot],
            device_id={"shard": peers[k]},
            device_id_type=MESH,
        )

    def block_copy(c, k, slot):
        a, col, width = chunks[c]
        block = finals[a].at[pl.ds(pl.multiple_of(slot * rows, rows), rows), pl.ds(col, width)]
        return pltpu.make_async_remote_copy(
            src_ref=block,
            dst_ref=block,
            send_sem=send_sem.at[c, k],
            recv_sem=recv_sem.at[c, slot],
            device_id={"shard": peers[k]},
            device_id_type=MESH,
        )

    factors = (
        pltpu.make_async_copy(mix_hbm, mix_ref, row_sem.at[0]),
        pltpu.make_async_copy(gain_hbm, gain_ref, row_sem.at[1]),
    )
    for copy in factors:
        copy.start()
    for c in range(len(chunks)):
        for copy in loads(c):
            copy.start(priority=1)

    barrier = pltpu.get_barrier_semaphore()
    for peer in peers:
        pl.semaphore_signal(barrier, inc=1, device_id={"shard": peer}, device_id_type=MESH)

    for copy in factors:
        copy.wait()
    for k in range(rows // LANES):
        mix = mix_ref[k : k + 1, :]
        gain = gain_ref[k : k + 1, :]
        span = pl.ds(k * LANES, LANES)
        first[span, :] = jnp.broadcast_to(mix * gain, (LANES, LANES)).T
        second[span, :] = jnp.broadcast_to((1.0 - mix) * gain, (LANES, LANES)).T

    pl.semaphore_wait(barrier, n - 1)

    def combine(c):
        a, col, width = chunks[c]
        for copy in loads(c):
            copy.wait()
        lanes = range(0, width, LANES)

        def step(i, peak):
            span = pl.ds(pl.multiple_of(i * BLOCK, BLOCK), BLOCK)
            one_factor, other_factor = first[span, :], second[span, :]
            tops = []
            for j, top in zip(lanes, peak):
                cols = pl.ds(col + j, LANES)
                value = one_factor * held[a][span, cols] + other_factor * extra[a][span, cols]
                held[a][span, cols] = value
                top_here = jnp.max(jnp.abs(value).reshape(BLOCK // 8, 8, LANES), axis=0)
                tops.append(jnp.maximum(top, top_here))
            return tuple(tops)

        zero = jnp.zeros((8, LANES), jnp.float32)
        tops = lax.fori_loop(0, rows // BLOCK, step, (zero,) * len(lanes))
        for j, top in zip(lanes, tops):
            peaks[c, me, :, j : j + LANES] = top
        for k in range(n - 1):
            peak_copy(c, k, me).start()

    def finish(c):
        a, col, width = chunks[c]
        cols = pl.ds(col, width)
        for k in range(n - 1):
            peak_copy(c, k, peers[k]).wait_recv()
        peak = peaks[c, 0, :, :width]
        for k in range(1, n):
            peak = jnp.maximum(peak, peaks[c, k, :, :width])
        scale = jnp.max(peak, axis=0, keepdims=True)
        for j in range(0, width, LANES):
            row = (col + j) // LANES
            scales[a][row : row + 1, :] = scale[:, j : j + LANES]
        inverse = 1.0 / scale

        def step(i, carry):
            span = pl.ds(pl.multiple_of(i * BLOCK, BLOCK), BLOCK)
            out = pl.ds(pl.multiple_of(me * rows + i * BLOCK, BLOCK), BLOCK)
            finals[a][out, cols] = (held[a][span, cols] * inverse).astype(jnp.bfloat16)
            return carry

        lax.fori_loop(0, rows // BLOCK, step, 0)
        for k in range(n - 1):
            block_copy(c, k, me).start()

    combine(0)
    for c in range(len(chunks)):
        if c + 1 < len(chunks):
            combine(c + 1)
        finish(c)
    for c in range(len(chunks)):
        for k in range(n - 1):
            peak_copy(c, k, me).wait_send()
            block_copy(c, k, me).wait_send()
            block_copy(c, k, peers[k]).wait_recv()


def write_out(*refs):
    half = (len(refs) - 1) // 2
    sem = refs[-1]
    copies = [
        pltpu.make_async_copy(refs[i], refs[half + i], sem.at[i]) for i in range(half)
    ]
    for copy in copies:
        copy.start()
    for copy in copies:
        copy.wait()


def cut(widths):
    chunks = []
    for a, total in enumerate(widths):
        col = 0
        while col < total:
            width = min(LANES if len(chunks) < NARROW else WIDTH, total - col)
            chunks.append((a, col, width))
            col += width
    return chunks


def shards(
    n, one_query, other_query, one_key, other_key, one_value, other_value, mix_share, norm_gain
):
    ones = (one_query, one_key, one_value)
    others = (other_query, other_key, other_value)
    rows = one_query.shape[0]
    chunks = cut([x.shape[1] for x in ones])
    count = len(chunks)
    vmem = pl.BlockSpec(memory_space=pltpu.VMEM)
    hbm = pl.BlockSpec(memory_space=pltpu.HBM)
    shapes = [((n * rows, x.shape[1]), jnp.bfloat16) for x in ones] + [
        ((x.shape[1] // LANES, LANES), jnp.float32) for x in ones
    ]
    scratch = (
        [pltpu.VMEM(x.shape, jnp.float32) for x in ones + others]
        + [pltpu.VMEM((rows // LANES, LANES), jnp.float32)] * 2
        + [pltpu.VMEM((rows, LANES), jnp.float32)] * 2
        + [
            pltpu.VMEM((count, n, 8, WIDTH), jnp.float32),
            pltpu.SemaphoreType.DMA((2,)),
            pltpu.SemaphoreType.DMA((count, 2)),
            pltpu.SemaphoreType.DMA((count, n - 1)),
            pltpu.SemaphoreType.DMA((count, n)),
            pltpu.SemaphoreType.DMA((count, n - 1)),
            pltpu.SemaphoreType.DMA((count, n)),
        ]
    )
    grant = sum(2 * x.size * 4 for x in ones) + 2 * rows * LANES * 4
    grant += count * n * 8 * WIDTH * 4 + (2 << 20)
    merged = pl.pallas_call(
        functools.partial(merge, n, chunks),
        out_shape=[pltpu.VMEM(s, d) for s, d in shapes],
        in_specs=[hbm] * 8,
        out_specs=[vmem] * 6,
        scratch_shapes=scratch,
        compiler_params=pltpu.CompilerParams(
            collective_id=0, has_side_effects=True, vmem_limit_bytes=grant
        ),
        name="merge",
    )(
        *(
            pltpu.with_memory_space_constraint(x, pltpu.HBM)
            for x in (
                *ones,
                *others,
                mix_share.reshape(rows // LANES, LANES),
                norm_gain.reshape(rows // LANES, LANES),
            )
        )
    )
    outs = pl.pallas_call(
        write_out,
        out_shape=[jax.ShapeDtypeStruct(s, d) for s, d in shapes],
        in_specs=[vmem] * 6,
        out_specs=[hbm] * 6,
        scratch_shapes=[pltpu.SemaphoreType.DMA((6,))],
        compiler_params=pltpu.CompilerParams(vmem_limit_bytes=1 << 20),
        name="write_out",
    )(*merged)
    return (*outs[:3], *(x.reshape(-1) for x in outs[3:]))


def solution(mesh):
    rows = P(("job", "shard"))
    blocks = P(("job", "shard"), "cols")
    return jax.shard_map(
        functools.partial(shards, mesh.shape["shard"]),
        mesh=mesh,
        in_specs=(blocks,) * 6 + (rows,) * 2,
        out_specs=(P("job", "cols"),) * 3 + (P(("job", "cols")),) * 3,
        check_vma=False,
    )
```
